512 devices in a mesh: grp: 16 (over y, core), mem: 32 (over x, z).
Axes of the slice: x: 4, y: 8, z: 8, core: 2. Of those that a mesh axis runs over, the one named last changes fastest.
Arguments:
- v_stack: bfloat16 [524288, 512], P(('grp', 'mem')), may hold values from -0.1875 to 0.1875
- u_stack: bfloat16 [524288, 512], P(('grp', 'mem')), may hold values from -0.25 to 0.25
- warm_start: bfloat16 [524288, 256], P(('grp', 'mem')), may hold values from -3 to 3
- observed: bfloat16 [524288, 256], P(('grp', 'mem')), may hold values from -12 to 12, as said below
- owners: int32 [512, 4], replicated, may hold values from 0 to 511, as said below
- tile_ranks: int32 [512, 4], P(('grp', 'mem')), may hold values from 8 to 128
Outputs:
- model: float32 [524288, 256], P(('grp', 'mem'))
- residual: bfloat16 [524288, 256], P(('grp', 'mem'))
The draws below stay inside these ranges and needn't reach their ends.
Inputs may be any that keep to these rules, and one draw needn't show every extreme that they name: Writing d = g * 32 + m, owners[d, t] = ((g + a_t) mod 16) * 32 + (m + b_t) mod 32, where the offsets a_t differ over t, the offsets b_t differ over t, some slot has a_t = 15, some slot has a_t = 8, some slot has b_t = 31 and some slot has b_t = 16. `observed`: entries of one row block share a scale.
All inputs are finite; a program needn't handle non-finite values.
Results may differ from the reference program's by a relative error of at most 0.006.
Values may be sent and summed in bfloat16 or wider, within the bound.
No kernel may reach another device: no remote copies, remote signals or barrier semaphores. Data moves between devices by JAX's collectives and lax.ppermute only.
A program may use at most 64 MiB of HBM per device.

```python
import jax
import jax.numpy as jnp
from jax import lax

BS = 1024
RMAX = 128
TPC = 4
RHS = 256
ITERS = 2
NORDER = 524288
N_GRP = 16
N_MEM = 32
DEVICES = 512


def offsets_with_top(key, count):
    first, second = jax.random.split(key, 2)
    half = count // 2
    rest = jax.random.permutation(first, count - 2).astype(jnp.int32)
    rest = jnp.where(rest < half, rest, rest + 1).astype(jnp.int32)
    chosen = jnp.concatenate([jnp.array([count - 1, half], dtype=jnp.int32), rest[:TPC - 2]])
    order = jax.random.permutation(second, TPC).astype(jnp.int32)
    return chosen[order].astype(jnp.int32)


def draw_owners(key, part):
    first, second = jax.random.split(jax.random.fold_in(key, 11), 2)
    leads = offsets_with_top(first, N_GRP)
    shifts = offsets_with_top(second, N_MEM)
    groups = jnp.arange(N_GRP, dtype=jnp.int32)[:, None]
    target_group = (groups + leads[None, :]) % N_GRP
    members = jnp.arange(N_MEM, dtype=jnp.int32)[:, None]
    target_member = (members + shifts[None, :]) % N_MEM
    owned = target_group[:, None, :] * N_MEM + target_member[None, :, :]
    return owned.reshape(N_GRP * N_MEM, TPC).astype(jnp.int32)


def draw_observed(key, part):
    first = jax.random.fold_in(jax.random.fold_in(key, 23), 0)
    rows = BS * DEVICES
    blocks = (jnp.arange(rows, dtype=jnp.int32) // BS).astype(jnp.float32)
    scales = 1.0 + 2.0 * blocks / max(DEVICES - 1, 1)
    values = jax.random.normal(first, (rows, RHS), jnp.float32) * scales[:, None]
    return jnp.clip(values, -12.0, 12.0).astype(jnp.bfloat16)


def with_ends(values, stream_key, least, high):
    spot = [jax.random.randint(jax.random.fold_in(stream_key, axis), (), 0, length) for axis, length in enumerate(values.shape)]
    longest = values.shape.index(max(values.shape))
    beside = spot[:longest] + [(spot[longest] + 1) % values.shape[longest]] + spot[longest + 1:]
    return values.at[tuple(spot)].set(least).at[tuple(beside)].set(high)


def block_levels(own_key, shape, shards, least, largest):
    factor_of, own = 1.0, jax.random.fold_in(own_key, 6)
    for dim, blocks in shards:
        draws = jnp.exp(jax.random.uniform(jax.random.fold_in(own, dim), (blocks,), jnp.float32, least / len(shards), largest / len(shards)))
        factor_of = factor_of * jnp.repeat(draws, shape[dim] // blocks).reshape([-1 if axis == dim else 1 for axis in range(len(shape))])
    return factor_of


def gaussian(rng, dims, spread, most, pieces=(), held_as=jnp.bfloat16):
    values = spread * jax.random.normal(rng, dims, jnp.float32)
    if pieces:
        values = values * block_levels(rng, dims, pieces, -0.22, 0.18)
    return jnp.clip(values, -most, most).astype(held_as)


def setup_inputs(seed: int = 0) -> dict:
    keys = jax.random.split(jax.random.key(seed), 7)
    v_stack = gaussian(keys[0], (NORDER, TPC * RMAX), BS ** -0.5, 0.1875, ((0, 512),))
    u_stack = gaussian(keys[1], (NORDER, TPC * RMAX), (TPC * RMAX) ** -0.5, 0.25, ((0, 512),))
    warm_start = gaussian(keys[2], (NORDER, RHS), 0.5, 3.0, ((0, 512),))
    observed = draw_observed(jax.random.fold_in(keys[6], 71), 0)
    owners = draw_owners(jax.random.fold_in(keys[6], 71), 0)
    tile_ranks = with_ends(jax.random.randint(keys[5], (DEVICES, TPC), RMAX // 16, RMAX + 1), jax.random.fold_in(keys[5], 1), RMAX // 16, RMAX).astype(jnp.int32)
    return {"v_stack": v_stack, "u_stack": u_stack, "warm_start": warm_start, "observed": observed, "owners": owners, "tile_ranks": tile_ranks}


def reference(v_stack, u_stack, warm_start, observed, owners, tile_ranks):
    right_bases = v_stack.reshape(DEVICES, BS, TPC * RMAX)
    left_bases = u_stack.reshape(DEVICES, BS, TPC * RMAX)
    live_rows = (jnp.arange(RMAX, dtype=jnp.int32)[None, None, :] < tile_ranks[:, :, None]).astype(jnp.float32)
    slot_ids = jnp.arange(TPC, dtype=jnp.int32)[None, :]
    column_ids = jnp.broadcast_to(jnp.arange(DEVICES, dtype=jnp.int32)[:, None], (DEVICES, TPC))
    sources = jnp.zeros((DEVICES, TPC), jnp.int32).at[owners, jnp.broadcast_to(slot_ids, (DEVICES, TPC))].set(column_ids)

    def right_product(pair):
        return jnp.dot(pair[0].T, pair[1], preferred_element_type=jnp.float32)

    def left_apply(pair):
        return jnp.dot(pair[0], pair[1].reshape(TPC * RMAX, RHS), preferred_element_type=jnp.float32)

    def forward(field):
        panels = lax.map(right_product, (right_bases, field)).reshape(DEVICES, TPC, RMAX, RHS)
        panels = (panels * live_rows[..., None]).astype(jnp.bfloat16)
        arrived = panels[sources, slot_ids]
        return lax.map(left_apply, (left_bases, arrived))

    def adjoint(field):
        panels = lax.map(right_product, (left_bases, field)).reshape(DEVICES, TPC, RMAX, RHS).astype(jnp.bfloat16)
        returned = panels[owners, slot_ids]
        masked = (returned * live_rows[..., None]).astype(jnp.bfloat16)
        return lax.map(left_apply, (right_bases, masked))

    start = warm_start.reshape(DEVICES, BS, RHS)
    model = start.astype(jnp.float32)
    residual = forward(start) - observed.reshape(DEVICES, BS, RHS).astype(jnp.float32)
    entries = float(NORDER * RHS)

    def iterate(index, carry):
        model, residual = carry
        huber_scale = 1.345 * jnp.sum(jnp.abs(residual)) / entries + 1e-6
        weights = huber_scale / jnp.maximum(jnp.abs(residual), huber_scale)
        weighted = (weights * residual).astype(jnp.bfloat16)
        gradient = adjoint(weighted)
        image_dir = forward(gradient.astype(jnp.bfloat16))
        step_size = jnp.sum(gradient * gradient) / (jnp.sum(weights * image_dir * image_dir) + 1e-6)
        return (model - step_size * gradient, residual - step_size * image_dir)

    model, residual = lax.fori_loop(0, ITERS, iterate, (model, residual))
    return model.reshape(NORDER, RHS), residual.reshape(NORDER, RHS).astype(jnp.bfloat16)
```

```python
import jax
import jax.numpy as jnp
from jax import lax
from jax.sharding import PartitionSpec as P

ITERS = 2
ALL = ("grp", "mem")


def total(values):
    k = values.shape[0]
    for axis in ALL:
        n = lax.axis_size(axis)
        spread = jnp.broadcast_to(values[None, :, None], (n, k, 128))
        got = lax.all_to_all(spread, axis, split_axis=0, concat_axis=0, tiled=True)
        values = jnp.sum(got[:, :, 0], axis=0)
    return values


def on_device(v_stack, u_stack, warm_start, observed, owners, tile_ranks):
    group_count = lax.axis_size("grp")
    member_count = lax.axis_size("mem")
    devices = group_count * member_count
    slots = owners.shape[1]
    width = v_stack.shape[1]
    rank_cap = width // slots
    rhs = warm_start.shape[1]
    live = (
        lax.broadcasted_iota(jnp.int32, (slots, rank_cap, 1), 1) < tile_ranks[0][:, None, None]
    ).reshape(width, 1)
    me = lax.axis_index(ALL)
    mine = lax.dynamic_index_in_dim(owners[0], me // (devices // slots), 0, keepdims=False)
    lead = mine // member_count
    shift = mine % member_count
    scatter = (lambda x: lax.all_to_all(x, ALL, split_axis=0, concat_axis=0, tiled=True))

    def route(panels, lead, shift):
        x = scatter(panels.reshape(devices, rhs // 128, 128))
        x = x.reshape(group_count, member_count, rhs // 128, 128)
        x = jnp.roll(x, (lead, shift), axis=(0, 1))
        x = scatter(x.reshape(devices, rhs // 128, 128))
        return x.reshape(width, rhs)

    def forward(field):
        panels = lax.dot_general(
            v_stack, field, (((0,), (0,)), ((), ())), preferred_element_type=jnp.float32
        )
        panels = jnp.where(live, panels, 0.0).astype(jnp.bfloat16)
        arrived = route(panels, lead, shift)
        return jnp.dot(u_stack, arrived, preferred_element_type=jnp.float32)

    def adjoint(field):
        panels = lax.dot_general(
            u_stack, field, (((0,), (0,)), ((), ())), preferred_element_type=jnp.float32
        ).astype(jnp.bfloat16)
        back = route(panels, (group_count - lead) % group_count, (member_count - shift) % member_count)
        back = jnp.where(live, back, jnp.zeros_like(back))
        return jnp.dot(v_stack, back, preferred_element_type=jnp.float32)

    model = warm_start.astype(jnp.float32)
    residual = forward(warm_start) - observed.astype(jnp.float32)
    entries = float(warm_start.shape[0] * rhs * devices)

    def iterate(_, carry):
        model, residual = carry
        spread = total(jnp.sum(jnp.abs(residual))[None])[0]
        scale = 1.345 * spread / entries + 1e-06
        weights = scale / jnp.maximum(jnp.abs(residual), scale)
        weighted = (weights * residual).astype(jnp.bfloat16)
        gradient = adjoint(weighted)
        image = forward(gradient.astype(jnp.bfloat16))
        sums = total(
            jnp.stack([jnp.sum(gradient * gradient), jnp.sum(weights * image * image)])
        )
        step = sums[0] / (sums[1] + 1e-06)
        model = model - step * gradient
        residual = residual - step * image
        return model, residual

    model, residual = lax.fori_loop(0, ITERS, iterate, (model, residual))
    return model, residual.astype(jnp.bfloat16)


def solution(mesh):
    rows = P(ALL, None)
    return jax.shard_map(
        on_device,
        mesh=mesh,
        in_specs=(rows, rows, rows, rows, P(), rows),
        out_specs=(rows, rows),
        check_vma=False,
    )
```

```python
import functools

import jax
import jax.numpy as jnp
from jax import lax
from jax.experimental import pallas as pl
from jax.experimental.pallas import tpu as pltpu
from jax.sharding import Mesh
from jax.sharding import PartitionSpec as P

ITERS = 2
ALL = ("y", "c", "x", "z")
GRP = ("y", "c")
MEM = ("x", "z")
CHIPS = ("y", "x", "z")
LANES = 128
QUAD = 4
F32 = jnp.float32
BF16 = jnp.bfloat16


def call(kernel, out_shape, in_spaces, scratch=(), flops=0, vmem_mib=12):
    spaces = {"v": pltpu.VMEM, "s": pltpu.SMEM}
    return pl.pallas_call(
        kernel,
        out_shape=out_shape,
        in_specs=[pl.BlockSpec(memory_space=spaces[s]) for s in in_spaces],
        out_specs=jax.tree.map(lambda _: pl.BlockSpec(memory_space=pltpu.VMEM), out_shape),
        scratch_shapes=list(scratch),
        compiler_params=pltpu.CompilerParams(vmem_limit_bytes=vmem_mib * 2**20),
        cost_estimate=pl.CostEstimate(flops=flops, bytes_accessed=2**20, transcendentals=0),
    )


def to_chunks(rows):
    halves = [
        rows[:, h * LANES : (h + 1) * LANES].reshape(rows.shape[0] // QUAD, QUAD, LANES)
        for h in range(rows.shape[1] // LANES)
    ]
    return halves


def from_chunks(ref):
    half = ref.shape[0] // 2
    parts = [ref[h * half : (h + 1) * half].reshape(half * QUAD, LANES) for h in range(2)]
    return jnp.concatenate(parts, axis=1)


def keep_live(rows, ranks_ref, cap):
    parts = []
    for t in range(rows.shape[0] // cap):
        part = rows[t * cap : (t + 1) * cap]
        row = lax.broadcasted_iota(jnp.int32, part.shape, 0)
        parts.append(jnp.where(row < ranks_ref[t], part, jnp.zeros_like(part)))
    return jnp.concatenate(parts, axis=0)


def put_chunks(out_ref, rows):
    half = out_ref.shape[0] // 2
    for h, part in enumerate(to_chunks(rows)):
        out_ref[h * half : (h + 1) * half] = part


def roll_kernel(outer, inner, sign, owner_ref, here_ref, own_ref, swapped_ref, out_ref):
    core = here_ref[0]
    owner = owner_ref[here_ref[1]]
    group = lax.div(owner, inner)
    odd = group & 1
    source = core ^ odd
    lead = ((source + sign * group) >> 1) & (outer - 1)
    shift = (sign * lax.rem(owner, inner)) & (inner - 1)

    def copy(src_ref):
        def rows(o, carry):
            base = ((o + lead) & (outer - 1)) * inner
            for i in range(inner):
                out_ref[base + ((i + shift) & (inner - 1))] = src_ref[o * inner + i]
            return carry

        lax.fori_loop(0, outer, rows, 0)

    @pl.when(odd == 0)
    def _():
        copy(own_ref)

    @pl.when(odd != 0)
    def _():
        copy(swapped_ref)


def spread_kernel(got_ref, out_ref):
    sums = jnp.sum(got_ref[...], axis=0, keepdims=True)
    out_ref[...] = jnp.broadcast_to(sums, out_ref.shape)


def huber_scale(sums_ref, entries):
    spread = jnp.sum(sums_ref[:, 0, :], axis=0, keepdims=True)
    return 1.345 * spread[:, 0:1] / entries + 1e-06


def first_kernel(chunks_ref, u_ref, observed_ref, residual_ref, sums_ref):
    arrived = from_chunks(chunks_ref)
    total = jnp.zeros((1, 1), F32)
    step = 256
    for i in range(0, u_ref.shape[0], step):
        rows = jnp.dot(u_ref[i : i + step], arrived, preferred_element_type=F32)
        rows = rows - observed_ref[i : i + step].astype(F32)
        residual_ref[i : i + step] = rows
        total = total + jnp.sum(jnp.abs(rows), keepdims=True)
    sums_ref[...] = jnp.broadcast_to(total[None], sums_ref.shape)


def weigh_kernel(entries, sums_ref, residual_ref, ut_ref, chunks_ref, weighted_ref):
    scale = huber_scale(sums_ref, entries)
    residual = residual_ref[...]
    weighted_ref[...] = (scale / jnp.maximum(jnp.abs(residual), scale) * residual).astype(BF16)
    step = 256
    parts = [
        jnp.dot(ut_ref[i : i + step], weighted_ref[...], preferred_element_type=F32).astype(BF16)
        for i in range(0, ut_ref.shape[0], step)
    ]
    put_chunks(chunks_ref, jnp.concatenate(parts, axis=0))


def gradient_kernel(
    cap, ranks_ref, chunks_ref, v_ref, vt_ref, gradient_ref, square_ref, out_ref, rounded_ref
):
    back = keep_live(from_chunks(chunks_ref), ranks_ref, cap)
    total = jnp.zeros((1, 1), F32)
    step = 256
    for i in range(0, v_ref.shape[0], step):
        rows = jnp.dot(v_ref[i : i + step], back, preferred_element_type=F32)
        gradient_ref[i : i + step] = rows
        rounded_ref[i : i + step] = rows.astype(BF16)
        total = total + jnp.sum(rows * rows, keepdims=True)
    square_ref[...] = jnp.broadcast_to(total, square_ref.shape)
    parts = [
        jnp.dot(vt_ref[i : i + step], rounded_ref[...], preferred_element_type=F32)
        for i in range(0, vt_ref.shape[0], step)
    ]
    put_chunks(out_ref, keep_live(jnp.concatenate(parts, axis=0), ranks_ref, cap).astype(BF16))


def image_kernel(entries, spread_ref, chunks_ref, u_ref, residual_ref, square_ref, image_ref, sums_ref):
    scale = huber_scale(spread_ref, entries)
    arrived = from_chunks(chunks_ref)
    total = jnp.zeros((1, 1), F32)
    step = 256
    for i in range(0, u_ref.shape[0], step):
        rows = jnp.dot(u_ref[i : i + step], arrived, preferred_element_type=F32)
        image_ref[i : i + step] = rows
        weights = scale / jnp.maximum(jnp.abs(residual_ref[i : i + step]), scale)
        total = total + jnp.sum(weights * rows * rows, keepdims=True)
    sums_ref[:, 0:1, :] = jnp.broadcast_to(square_ref[0:1, :][None], (sums_ref.shape[0], 1, LANES))
    sums_ref[:, 1:2, :] = jnp.broadcast_to(total[None], (sums_ref.shape[0], 1, LANES))


def step_of(sums_ref):
    grad = jnp.sum(sums_ref[:, 0, :], axis=0, keepdims=True)[:, 0:1]
    curve = jnp.sum(sums_ref[:, 1, :], axis=0, keepdims=True)[:, 0:1]
    return grad / (curve + 1e-06)


def update_kernel(sums_ref, residual_ref, image_ref, out_ref, step_ref, spread_ref):
    step = step_of(sums_ref)
    residual = residual_ref[...] - step * image_ref[...]
    out_ref[...] = residual
    step_ref[...] = jnp.broadcast_to(step, step_ref.shape)
    total = jnp.sum(jnp.abs(residual), keepdims=True)
    spread_ref[...] = jnp.broadcast_to(total[None], spread_ref.shape)


def last_kernel(sums_ref, residual_ref, image_ref, start_ref, gradient_ref, *rest):
    earlier, (out_ref, residual_out_ref) = rest[:-2], rest[-2:]
    step = step_of(sums_ref)
    model = start_ref[...].astype(F32)
    for k in range(0, len(earlier), 2):
        model = model - earlier[k][0:1, 0:1] * earlier[k + 1][...]
    out_ref[...] = model - step * gradient_ref[...]
    residual_out_ref[...] = (residual_ref[...] - step * image_ref[...]).astype(BF16)


def on_device(v_stack, u_stack, warm_start, observed, owners, tile_ranks):
    groups = lax.axis_size(GRP)
    members = lax.axis_size(MEM)
    rows_of_chips = lax.axis_size("y")
    chips = rows_of_chips * members
    slots = owners.shape[1]
    block, width = v_stack.shape
    cap = width // slots
    rhs = warm_start.shape[1]
    entries = float(block * rhs * groups * members)
    ranks = tile_ranks[0]
    struct = jax.ShapeDtypeStruct
    chunked = struct((chips, QUAD, LANES), BF16)
    field = struct((block, rhs), F32)
    flops = 2 * block * width * rhs

    per_slot = chips // 2 // slots
    slot = lax.axis_index(CHIPS) % (chips // 2) // per_slot
    here = jnp.stack([lax.axis_index("c"), slot])
    owner = owners[0]

    def scatter(x, axes):
        return lax.all_to_all(x, axes, split_axis=0, concat_axis=0, tiled=True)

    def route(chunks, sign):
        got = scatter(chunks, CHIPS)
        swapped = lax.ppermute(got, "c", [(0, 1), (1, 0)])
        rolled = call(
            functools.partial(roll_kernel, rows_of_chips, members, sign),
            chunked,
            "ssvv",
            flops=10**8,
        )(owner, here, got, swapped)
        return scatter(rolled, CHIPS)

    def total(partial):
        got = scatter(partial, GRP)
        kinds = partial.shape[1]
        spread = call(spread_kernel, struct((members, kinds, LANES), F32), "v")(got)
        return scatter(spread, MEM)

    live = (
        lax.broadcasted_iota(jnp.int32, (slots, cap, 1), 1) < ranks[:, None, None]
    ).reshape(width, 1)
    vt = v_stack.T
    ut = u_stack.T

    panels = lax.dot_general(
        v_stack, warm_start, (((0,), (0,)), ((), ())), preferred_element_type=F32
    )
    panels = jnp.where(live, panels, 0.0).astype(BF16)
    chunks = jnp.concatenate(to_chunks(panels), axis=0)
    one = struct((groups, 1, LANES), F32)
    two = struct((groups, 2, LANES), F32)
    residual, partial = call(first_kernel, (field, one), "vvv", flops=flops)(
        route(chunks, 1), u_stack, observed
    )
    earlier = []
    for index in range(ITERS):
        spread = total(partial)
        chunks = call(
            functools.partial(weigh_kernel, entries),
            chunked,
            "vvv",
            [pltpu.VMEM((block, rhs), BF16)],
            flops=flops,
        )(spread, residual, ut)
        gradient, square, chunks = call(
            functools.partial(gradient_kernel, cap),
            (field, struct((8, LANES), F32), chunked),
            "svvv",
            [pltpu.VMEM((block, rhs), BF16)],
            flops=2 * flops,
        )(ranks, route(chunks, -1), v_stack, vt)
        image, partial = call(
            functools.partial(image_kernel, entries), (field, two), "vvvvv", flops=flops
        )(spread, route(chunks, 1), u_stack, residual, square)
        sums = total(partial)
        if index < ITERS - 1:
            residual, step, partial = call(
                update_kernel, (field, struct((8, LANES), F32), one), "vvv"
            )(sums, residual, image)
            earlier += [step, gradient]
        else:
            model, residual = call(
                last_kernel, (field, struct((block, rhs), BF16)), "v" * (5 + len(earlier))
            )(sums, residual, image, warm_start, gradient, *earlier)
    return model, residual


def solution(mesh):
    finer = Mesh(mesh.devices.reshape(8, 2, 4, 8), ALL)
    rows = P(ALL, None)
    return jax.shard_map(
        on_device,
        mesh=finer,
        in_specs=(rows, rows, rows, rows, P(), rows),
        out_specs=(rows, rows),
        check_vma=False,
    )
```

```python
import functools

import jax
import jax.numpy as jnp
from jax import lax
from jax.experimental import pallas as pl
from jax.experimental.pallas import tpu as pltpu
from jax.sharding import Mesh
from jax.sharding import PartitionSpec as P

ITERS = 2
ALL = ("y", "c", "x", "z")
GRP = ("y", "c")
MEM = ("x", "z")
LANES = 128
PAIR = 2
F32 = jnp.float32
BF16 = jnp.bfloat16


def call(kernel, out_shape, in_spaces, scratch=(), flops=0, vmem_mib=12):
    spaces = {"v": pltpu.VMEM, "s": pltpu.SMEM}
    return pl.pallas_call(
        kernel,
        out_shape=out_shape,
        in_specs=[pl.BlockSpec(memory_space=spaces[s]) for s in in_spaces],
        out_specs=jax.tree.map(lambda _: pl.BlockSpec(memory_space=pltpu.VMEM), out_shape),
        scratch_shapes=list(scratch),
        compiler_params=pltpu.CompilerParams(vmem_limit_bytes=vmem_mib * 2**20),
        cost_estimate=pl.CostEstimate(flops=flops, bytes_accessed=2**20, transcendentals=0),
    )


def panel_of(ref, slot, cap, kind, column):
    pairs = cap // PAIR
    slots = ref.shape[0] // (2 * pairs)
    first = ((column % 2) * slots + slot) * pairs
    return ref[first : first + pairs, kind + column // 2].reshape(cap, LANES)


def rows_of(ref, slot, cap, kind, columns):
    return jnp.concatenate([panel_of(ref, slot, cap, kind, c) for c in range(columns)], axis=1)


def put_pieces(out_ref, first, rows):
    half = out_ref.shape[0] // 2
    pairs = rows.shape[0] // PAIR
    for h in range(2):
        piece = rows[:, h * LANES : (h + 1) * LANES].reshape(pairs, PAIR, LANES)
        out_ref[h * half + first : h * half + first + pairs] = piece


def move(outer, inner, leads, shifts, src_ref, put, double_ref):
    def widen(o, carry):
        rows = src_ref[pl.ds(o * inner, inner)]
        double_ref[pl.ds(2 * o * inner, inner)] = rows
        double_ref[pl.ds((2 * o + 1) * inner, inner)] = rows
        return carry

    lax.fori_loop(0, outer, widen, 0)

    def rows(o, carry):
        for k, (lead, shift) in enumerate(zip(leads, shifts)):
            start = 2 * o * inner + ((inner - shift) & (inner - 1))
            put(k, ((o + lead) & (outer - 1)) * inner, double_ref[pl.ds(start, inner)])
        return carry

    lax.fori_loop(0, outer, rows, 0)


def deliver_kernel(outer, inner, owner_ref, here_ref, src_ref, out_ref, double_ref):
    owner = owner_ref[here_ref[0]]

    def put(k, first, rows):
        out_ref[pl.ds(first, inner)] = rows

    move(
        outer, inner, [lax.div(owner, inner)], [lax.rem(owner, inner)], src_ref, put, double_ref
    )


def exchange_kernel(outer, inner, slots, owner_ref, here_ref, src_ref, out_ref, double_ref):
    slot = here_ref[0]
    group = lax.div(owner_ref[slot], inner)
    member = lax.rem(owner_ref[slot], inner)
    leads = [outer - group]
    shifts = [inner - member]
    for k in range(1, slots):
        other = owner_ref[lax.rem(slot + k, slots)]
        leads.append(lax.div(other, inner) - group + outer)
        shifts.append((lax.rem(other, inner) - member + inner) & (inner - 1))

    def put(k, first, rows):
        out_ref[pl.ds(first, inner), k] = rows

    move(outer, inner, leads, shifts, src_ref, put, double_ref)


def keep_live(rows, limit):
    row = lax.broadcasted_iota(jnp.int32, rows.shape, 0)
    return jnp.where(row < limit, rows, jnp.zeros_like(rows))


def spread_kernel(got_ref, out_ref):
    sums = jnp.sum(got_ref[...], axis=0, keepdims=True)
    out_ref[...] = jnp.broadcast_to(sums, out_ref.shape)


def huber_scale(sums_ref, entries):
    spread = jnp.sum(sums_ref[:, 0, :], axis=0, keepdims=True)
    return 1.345 * spread[:, 0:1] / entries + 1e-06


def first_kernel(
    cap, pieces_ref, u_ref, observed_ref, residual_ref, sums_ref, gram_ref, arrived_ref
):
    for t in range(u_ref.shape[1] // cap):
        arrived_ref[t * cap : (t + 1) * cap] = rows_of(pieces_ref, t, cap, 0, 2)
        gram_ref[t * cap : (t + 1) * cap] = rows_of(pieces_ref, t, cap, 1, gram_ref.shape[1] // LANES)
    total = jnp.zeros((1, 1), F32)
    step = 256
    for i in range(0, u_ref.shape[0], step):
        rows = jnp.dot(u_ref[i : i + step], arrived_ref[...], preferred_element_type=F32)
        rows = rows - observed_ref[i : i + step].astype(F32)
        residual_ref[i : i + step] = rows
        total = total + jnp.sum(jnp.abs(rows), keepdims=True)
    sums_ref[...] = jnp.broadcast_to(total[None], sums_ref.shape)


def weigh_kernel(entries, sums_ref, residual_ref, ut_ref, pieces_ref, own_ref, weighted_ref):
    scale = huber_scale(sums_ref, entries)
    residual = residual_ref[...]
    weighted_ref[...] = (scale / jnp.maximum(jnp.abs(residual), scale) * residual).astype(BF16)
    step = 256
    for i in range(0, ut_ref.shape[0], step):
        rows = jnp.dot(ut_ref[i : i + step], weighted_ref[...], preferred_element_type=F32)
        rows = rows.astype(BF16)
        own_ref[i : i + step] = rows
        put_pieces(pieces_ref, i // PAIR, rows)


def iterate_kernel(
    cap,
    entries,
    ranks_ref,
    spread_ref,
    pieces_ref,
    own_ref,
    gram_ref,
    v_ref,
    u_ref,
    residual_ref,
    gradient_ref,
    image_ref,
    sums_ref,
    back_ref,
    around_ref,
    panels_ref,
):
    slots = v_ref.shape[1] // cap
    step = 256
    for t in range(slots):
        back_ref[t * cap : (t + 1) * cap] = keep_live(rows_of(pieces_ref, t, cap, 0, 2), ranks_ref[t])
    grad = jnp.zeros((1, 1), F32)
    for i in range(0, v_ref.shape[0], step):
        rows = jnp.dot(v_ref[i : i + step], back_ref[...], preferred_element_type=F32)
        gradient_ref[i : i + step] = rows
        grad = grad + jnp.sum(rows * rows, keepdims=True)
    for mine in range(slots):
        for t in range(slots):
            kind = (mine - t) % slots
            if kind == 0:
                around_ref[t * cap : (t + 1) * cap] = own_ref[t * cap : (t + 1) * cap]
            else:
                around_ref[t * cap : (t + 1) * cap] = rows_of(pieces_ref, t, cap, kind, 2)
        panels_ref[mine * cap : (mine + 1) * cap] = jnp.dot(
            gram_ref[mine * cap : (mine + 1) * cap], around_ref[...], preferred_element_type=F32
        ).astype(BF16)
    scale = huber_scale(spread_ref, entries)
    curve = jnp.zeros((1, 1), F32)
    for i in range(0, u_ref.shape[0], step):
        rows = jnp.dot(u_ref[i : i + step], panels_ref[...], preferred_element_type=F32)
        image_ref[i : i + step] = rows
        weights = scale / jnp.maximum(jnp.abs(residual_ref[i : i + step]), scale)
        curve = curve + jnp.sum(weights * rows * rows, keepdims=True)
    sums_ref[:, 0:1, :] = jnp.broadcast_to(grad[None], (sums_ref.shape[0], 1, LANES))
    sums_ref[:, 1:2, :] = jnp.broadcast_to(curve[None], (sums_ref.shape[0], 1, LANES))


def step_of(sums_ref):
    grad = jnp.sum(sums_ref[:, 0, :], axis=0, keepdims=True)[:, 0:1]
    curve = jnp.sum(sums_ref[:, 1, :], axis=0, keepdims=True)[:, 0:1]
    return grad / (curve + 1e-06)


def update_kernel(sums_ref, residual_ref, image_ref, out_ref, step_ref, spread_ref):
    step = step_of(sums_ref)
    residual = residual_ref[...] - step * image_ref[...]
    out_ref[...] = residual
    step_ref[...] = jnp.broadcast_to(step, step_ref.shape)
    total = jnp.sum(jnp.abs(residual), keepdims=True)
    spread_ref[...] = jnp.broadcast_to(total[None], spread_ref.shape)


def last_kernel(sums_ref, residual_ref, image_ref, start_ref, gradient_ref, *rest):
    earlier, (out_ref, residual_out_ref) = rest[:-2], rest[-2:]
    step = step_of(sums_ref)
    model = start_ref[...].astype(F32)
    for k in range(0, len(earlier), 2):
        model = model - earlier[k][0:1, 0:1] * earlier[k + 1][...]
    out_ref[...] = model - step * gradient_ref[...]
    residual_out_ref[...] = (residual_ref[...] - step * image_ref[...]).astype(BF16)


def on_device(v_stack, u_stack, warm_start, observed, owners, tile_ranks):
    groups = lax.axis_size(GRP)
    members = lax.axis_size(MEM)
    devices = groups * members
    slots = owners.shape[1]
    block, width = v_stack.shape
    cap = width // slots
    rhs = warm_start.shape[1]
    entries = float(block * rhs * groups * members)
    ranks = tile_ranks[0]
    struct = jax.ShapeDtypeStruct
    field = struct((block, rhs), F32)
    rounded = struct((block, rhs), BF16)
    panels_shape = struct((width, rhs), BF16)
    piece = (PAIR, LANES)
    flops = 2 * block * width * rhs

    half = devices // 2
    slot = lax.axis_index(ALL) % half // (half // slots)
    here = slot[None]
    owner = owners[0]

    def scatter(x, axes):
        return lax.all_to_all(x, axes, split_axis=0, concat_axis=0, tiled=True)

    def route(kernel, pieces, out):
        got = scatter(pieces, ALL)
        moved = call(
            functools.partial(kernel, groups, members),
            struct((devices,) + out, BF16),
            "ssv",
            [pltpu.VMEM((2 * devices,) + pieces.shape[1:], BF16)],
            flops=10**8,
        )(owner, here, got)
        return scatter(moved, ALL)

    def total(partial):
        got = scatter(partial, GRP)
        kinds = partial.shape[1]
        spread = call(spread_kernel, struct((members, kinds, LANES), F32), "v")(got)
        return scatter(spread, MEM)

    live = (
        lax.broadcasted_iota(jnp.int32, (slots, cap), 1) < ranks[:, None]
    ).reshape(width)
    ut = u_stack.T
    products = lax.dot_general(
        v_stack,
        jnp.concatenate([warm_start, v_stack], axis=1),
        (((0,), (0,)), ((), ())),
        preferred_element_type=F32,
    )
    columns = jnp.concatenate([jnp.ones((rhs,), jnp.bool_), live])
    products = jnp.where(live[:, None] & columns[None, :], products, 0.0).astype(BF16)
    kinds = (rhs + width) // (2 * LANES)
    pieces = (
        products.reshape(width // PAIR, PAIR, kinds, 2, LANES)
        .transpose(3, 0, 2, 1, 4)
        .reshape((devices, kinds) + piece)
    )
    one = struct((groups, 1, LANES), F32)
    two = struct((groups, 2, LANES), F32)
    residual, partial, gram = call(
        functools.partial(first_kernel, cap),
        (field, one, struct((width, width), BF16)),
        "vvv",
        [pltpu.VMEM((width, rhs), BF16)],
        flops=flops,
    )(route(deliver_kernel, pieces, (kinds,) + piece), u_stack, observed)
    exchange = lambda outer, inner, *refs: exchange_kernel(outer, inner, slots, *refs)
    earlier = []
    for index in range(ITERS):
        spread = total(partial)
        pieces, own = call(
            functools.partial(weigh_kernel, entries),
            (struct((devices,) + piece, BF16), panels_shape),
            "vvv",
            [pltpu.VMEM((block, rhs), BF16)],
            flops=flops,
        )(spread, residual, ut)
        gradient, image, partial = call(
            functools.partial(iterate_kernel, cap, entries),
            (field, field, two),
            "svvvvvvv",
            [pltpu.VMEM((width, rhs), BF16)] * 3,
            flops=3 * flops,
        )(
            ranks,
            spread,
            route(exchange, pieces, (slots,) + piece),
            own,
            gram,
            v_stack,
            u_stack,
            residual,
        )
        sums = total(partial)
        if index < ITERS - 1:
            residual, step, partial = call(
                update_kernel, (field, struct((8, LANES), F32), one), "vvv"
            )(sums, residual, image)
            earlier += [step, gradient]
        else:
            model, residual = call(last_kernel, (field, rounded), "v" * (5 + len(earlier)))(
                sums, residual, image, warm_start, gradient, *earlier
            )
    return model, residual


def solution(mesh):
    finer = Mesh(mesh.devices.reshape(8, 2, 4, 8), ALL)
    rows = P(ALL, None)
    return jax.shard_map(
        on_device,
        mesh=finer,
        in_specs=(rows, rows, rows, rows, P(), rows),
        out_specs=(rows, rows),
        check_vma=False,
    )
```

```python
import functools

import jax
import jax.numpy as jnp
from jax import lax
from jax.experimental import pallas as pl
from jax.experimental.pallas import tpu as pltpu
from jax.sharding import Mesh
from jax.sharding import PartitionSpec as P

ITERS = 2
ALL = ("y", "c", "x", "z")
GRP = ("y", "c")
MEM = ("x", "z")
LANES = 128
PAIR = 2
F32 = jnp.float32
BF16 = jnp.bfloat16


def call(kernel, out_shape, in_spaces, scratch=(), flops=0, vmem_mib=12):
    spaces = {"v": pltpu.VMEM, "s": pltpu.SMEM}
    return pl.pallas_call(
        kernel,
        out_shape=out_shape,
        in_specs=[pl.BlockSpec(memory_space=spaces[s]) for s in in_spaces],
        out_specs=jax.tree.map(lambda _: pl.BlockSpec(memory_space=pltpu.VMEM), out_shape),
        scratch_shapes=list(scratch),
        compiler_params=pltpu.CompilerParams(vmem_limit_bytes=vmem_mib * 2**20),
        cost_estimate=pl.CostEstimate(flops=flops, bytes_accessed=2**20, transcendentals=0),
    )


def panel_of(ref, slot, cap, kind, column):
    pairs = cap // PAIR
    slots = ref.shape[0] // (2 * pairs)
    first = ((column % 2) * slots + slot) * pairs
    return ref[first : first + pairs, kind + column // 2].reshape(cap, LANES)


def rows_of(ref, slot, cap, kind, columns):
    return jnp.concatenate([panel_of(ref, slot, cap, kind, c) for c in range(columns)], axis=1)


def put_pieces(out_ref, first, rows):
    half = out_ref.shape[0] // 2
    pairs = rows.shape[0] // PAIR
    for h in range(2):
        piece = rows[:, h * LANES : (h + 1) * LANES].reshape(pairs, PAIR, LANES)
        out_ref[h * half + first : h * half + first + pairs] = piece


def move(outer, inner, leads, shifts, src_ref, put, double_ref):
    def widen(o, carry):
        rows = src_ref[pl.ds(o * inner, inner)]
        double_ref[pl.ds(2 * o * inner, inner)] = rows
        double_ref[pl.ds((2 * o + 1) * inner, inner)] = rows
        return carry

    lax.fori_loop(0, outer, widen, 0)

    def rows(o, carry):
        for k, (lead, shift) in enumerate(zip(leads, shifts)):
            start = 2 * o * inner + ((inner - shift) & (inner - 1))
            put(k, ((o + lead) & (outer - 1)) * inner, double_ref[pl.ds(start, inner)])
        return carry

    lax.fori_loop(0, outer, rows, 0)


def deliver_kernel(outer, inner, owner_ref, here_ref, src_ref, out_ref, double_ref):
    owner = owner_ref[here_ref[0]]

    def put(k, first, rows):
        out_ref[pl.ds(first, inner)] = rows

    move(
        outer, inner, [lax.div(owner, inner)], [lax.rem(owner, inner)], src_ref, put, double_ref
    )


def exchange_kernel(outer, inner, slots, owner_ref, here_ref, src_ref, out_ref, double_ref):
    slot = here_ref[0]
    group = lax.div(owner_ref[slot], inner)
    member = lax.rem(owner_ref[slot], inner)
    leads = [outer - group]
    shifts = [inner - member]
    for k in range(1, slots):
        other = owner_ref[lax.rem(slot + k, slots)]
        leads.append(lax.div(other, inner) - group + outer)
        shifts.append((lax.rem(other, inner) - member + inner) & (inner - 1))

    def put(k, first, rows):
        out_ref[pl.ds(first, inner), k] = rows

    move(outer, inner, leads, shifts, src_ref, put, double_ref)


def keep_live(rows, limit):
    row = lax.broadcasted_iota(jnp.int32, rows.shape, 0)
    return jnp.where(row < limit, rows, jnp.zeros_like(rows))


def spread_kernel(got_ref, out_ref):
    sums = jnp.sum(got_ref[...], axis=0, keepdims=True)
    out_ref[...] = jnp.broadcast_to(sums, out_ref.shape)


def huber_scale(sums_ref, entries):
    spread = jnp.sum(sums_ref[:, 0, :], axis=0, keepdims=True)
    return 1.345 * spread[:, 0:1] / entries + 1e-06


def start_kernel(cap, ranks_ref, v_ref, warm_ref, pieces_ref):
    slots = v_ref.shape[1] // cap
    kinds = pieces_ref.shape[1]
    half = pieces_ref.shape[0] // 2
    pairs = cap // PAIR
    for t in range(slots):
        vt = v_ref[:, t * cap : (t + 1) * cap].T
        for kind in range(kinds):
            if kind == 0:
                right = warm_ref[...]
            else:
                right = v_ref[:, (kind - 1) * 2 * LANES : kind * 2 * LANES]
            rows = keep_live(jnp.dot(vt, right, preferred_element_type=F32), ranks_ref[t])
            for h in range(2):
                part = rows[:, h * LANES : (h + 1) * LANES]
                if kind > 0:
                    column = ((kind - 1) * 2 + h) * LANES
                    lane = lax.broadcasted_iota(jnp.int32, part.shape, 1) + column % cap
                    part = jnp.where(lane < ranks_ref[column // cap], part, jnp.zeros_like(part))
                first = h * half + t * pairs
                pieces_ref[first : first + pairs, kind] = part.astype(BF16).reshape(pairs, PAIR, LANES)


def first_kernel(
    cap, pieces_ref, u_ref, observed_ref, residual_ref, sums_ref, gram_ref, ut_ref, arrived_ref
):
    ut_ref[...] = u_ref[...].T
    for t in range(u_ref.shape[1] // cap):
        arrived_ref[t * cap : (t + 1) * cap] = rows_of(pieces_ref, t, cap, 0, 2)
        gram_ref[t * cap : (t + 1) * cap] = rows_of(pieces_ref, t, cap, 1, gram_ref.shape[1] // LANES)
    total = jnp.zeros((1, 1), F32)
    step = 256
    for i in range(0, u_ref.shape[0], step):
        rows = jnp.dot(u_ref[i : i + step], arrived_ref[...], preferred_element_type=F32)
        rows = rows - observed_ref[i : i + step].astype(F32)
        residual_ref[i : i + step] = rows
        total = total + jnp.sum(jnp.abs(rows), keepdims=True)
    sums_ref[...] = jnp.broadcast_to(total[None], sums_ref.shape)


def weigh_kernel(entries, sums_ref, residual_ref, ut_ref, pieces_ref, own_ref, weighted_ref):
    scale = huber_scale(sums_ref, entries)
    residual = residual_ref[...]
    weighted_ref[...] = (scale / jnp.maximum(jnp.abs(residual), scale) * residual).astype(BF16)
    step = 256
    for i in range(0, ut_ref.shape[0], step):
        rows = jnp.dot(ut_ref[i : i + step], weighted_ref[...], preferred_element_type=F32)
        rows = rows.astype(BF16)
        own_ref[i : i + step] = rows
        put_pieces(pieces_ref, i // PAIR, rows)


def iterate_kernel(
    cap,
    entries,
    ranks_ref,
    spread_ref,
    pieces_ref,
    own_ref,
    gram_ref,
    v_ref,
    u_ref,
    residual_ref,
    gradient_ref,
    image_ref,
    sums_ref,
    back_ref,
    around_ref,
    panels_ref,
):
    slots = v_ref.shape[1] // cap
    step = 256
    for t in range(slots):
        back_ref[t * cap : (t + 1) * cap] = keep_live(rows_of(pieces_ref, t, cap, 0, 2), ranks_ref[t])
    grad = jnp.zeros((1, 1), F32)
    for i in range(0, v_ref.shape[0], step):
        rows = jnp.dot(v_ref[i : i + step], back_ref[...], preferred_element_type=F32)
        gradient_ref[i : i + step] = rows
        grad = grad + jnp.sum(rows * rows, keepdims=True)
    for mine in range(slots):
        for t in range(slots):
            kind = (mine - t) % slots
            if kind == 0:
                around_ref[t * cap : (t + 1) * cap] = own_ref[t * cap : (t + 1) * cap]
            else:
                around_ref[t * cap : (t + 1) * cap] = rows_of(pieces_ref, t, cap, kind, 2)
        panels_ref[mine * cap : (mine + 1) * cap] = jnp.dot(
            gram_ref[mine * cap : (mine + 1) * cap], around_ref[...], preferred_element_type=F32
        ).astype(BF16)
    scale = huber_scale(spread_ref, entries)
    curve = jnp.zeros((1, 1), F32)
    for i in range(0, u_ref.shape[0], step):
        rows = jnp.dot(u_ref[i : i + step], panels_ref[...], preferred_element_type=F32)
        image_ref[i : i + step] = rows
        weights = scale / jnp.maximum(jnp.abs(residual_ref[i : i + step]), scale)
        curve = curve + jnp.sum(weights * rows * rows, keepdims=True)
    lane = lax.broadcasted_iota(jnp.int32, sums_ref.shape, 2)
    sums_ref[...] = jnp.where(lane < LANES // 2, grad[None], curve[None])


def step_of(sums_ref):
    sums = jnp.sum(sums_ref[:, 0, :], axis=0, keepdims=True)
    return sums[:, 0:1] / (sums[:, LANES // 2 : LANES // 2 + 1] + 1e-06)


def update_kernel(sums_ref, residual_ref, image_ref, out_ref, step_ref, spread_ref):
    step = step_of(sums_ref)
    residual = residual_ref[...] - step * image_ref[...]
    out_ref[...] = residual
    step_ref[...] = jnp.broadcast_to(step, step_ref.shape)
    total = jnp.sum(jnp.abs(residual), keepdims=True)
    spread_ref[...] = jnp.broadcast_to(total[None], spread_ref.shape)


def last_kernel(sums_ref, residual_ref, image_ref, start_ref, gradient_ref, *rest):
    earlier, (out_ref, residual_out_ref) = rest[:-2], rest[-2:]
    step = step_of(sums_ref)
    model = start_ref[...].astype(F32)
    for k in range(0, len(earlier), 2):
        model = model - earlier[k][0:1, 0:1] * earlier[k + 1][...]
    out_ref[...] = model - step * gradient_ref[...]
    residual_out_ref[...] = (residual_ref[...] - step * image_ref[...]).astype(BF16)


def on_device(v_stack, u_stack, warm_start, observed, owners, tile_ranks):
    groups = lax.axis_size(GRP)
    members = lax.axis_size(MEM)
    devices = groups * members
    slots = owners.shape[1]
    block, width = v_stack.shape
    cap = width // slots
    rhs = warm_start.shape[1]
    entries = float(block * rhs * groups * members)
    ranks = tile_ranks[0]
    struct = jax.ShapeDtypeStruct
    field = struct((block, rhs), F32)
    rounded = struct((block, rhs), BF16)
    panels_shape = struct((width, rhs), BF16)
    piece = (PAIR, LANES)
    flops = 2 * block * width * rhs

    half = devices // 2
    slot = lax.axis_index(ALL) % half // (half // slots)
    here = slot[None]
    owner = owners[0]

    def scatter(x, axes):
        return lax.all_to_all(x, axes, split_axis=0, concat_axis=0, tiled=True)

    def route(kernel, pieces, out):
        got = scatter(pieces, ALL)
        moved = call(
            functools.partial(kernel, groups, members),
            struct((devices,) + out, BF16),
            "ssv",
            [pltpu.VMEM((2 * devices,) + pieces.shape[1:], BF16)],
            flops=10**8,
        )(owner, here, got)
        return scatter(moved, ALL)

    def total(partial):
        got = scatter(partial, GRP)
        spread = call(spread_kernel, struct((members, 1, LANES), F32), "v")(got)
        return scatter(spread, MEM)

    kinds = (rhs + width) // (2 * LANES)
    pieces = call(
        functools.partial(start_kernel, cap),
        struct((devices, kinds) + piece, BF16),
        "svv",
        flops=3 * flops,
    )(ranks, v_stack, warm_start)
    one = struct((groups, 1, LANES), F32)
    residual, partial, gram, ut = call(
        functools.partial(first_kernel, cap),
        (field, one, struct((width, width), BF16), struct((width, block), BF16)),
        "vvv",
        [pltpu.VMEM((width, rhs), BF16)],
        flops=flops,
    )(route(deliver_kernel, pieces, (kinds,) + piece), u_stack, observed)
    exchange = lambda outer, inner, *refs: exchange_kernel(outer, inner, slots, *refs)
    earlier = []
    for index in range(ITERS):
        spread = total(partial)
        pieces, own = call(
            functools.partial(weigh_kernel, entries),
            (struct((devices,) + piece, BF16), panels_shape),
            "vvv",
            [pltpu.VMEM((block, rhs), BF16)],
            flops=flops,
        )(spread, residual, ut)
        gradient, image, partial = call(
            functools.partial(iterate_kernel, cap, entries),
            (field, field, one),
            "svvvvvvv",
            [pltpu.VMEM((width, rhs), BF16)] * 3,
            flops=3 * flops,
        )(
            ranks,
            spread,
            route(exchange, pieces, (slots,) + piece),
            own,
            gram,
            v_stack,
            u_stack,
            residual,
        )
        sums = total(partial)
        if index < ITERS - 1:
            residual, step, partial = call(
                update_kernel, (field, struct((8, LANES), F32), one), "vvv"
            )(sums, residual, image)
            earlier += [step, gradient]
        else:
            model, residual = call(last_kernel, (field, rounded), "v" * (5 + len(earlier)))(
                sums, residual, image, warm_start, gradient, *earlier
            )
    return model, residual


def solution(mesh):
    finer = Mesh(mesh.devices.reshape(8, 2, 4, 8), ALL)
    rows = P(ALL, None)
    return jax.shard_map(
        on_device,
        mesh=finer,
        in_specs=(rows, rows, rows, rows, P(), rows),
        out_specs=(rows, rows),
        check_vma=False,
    )
```

```python
import functools

import jax
import jax.numpy as jnp
from jax import lax
from jax.experimental import pallas as pl
from jax.experimental.pallas import tpu as pltpu
from jax.sharding import Mesh
from jax.sharding import PartitionSpec as P

ITERS = 2
ALL = ("y", "c", "x", "z")
GRP = ("y", "c")
MEM = ("x", "z")
LANES = 128
PAIR = 2
F32 = jnp.float32
BF16 = jnp.bfloat16


def call(kernel, out_shape, in_spaces, scratch=(), flops=0, vmem_mib=12):
    spaces = {"v": pltpu.VMEM, "s": pltpu.SMEM, "h": pltpu.HBM}
    return pl.pallas_call(
        kernel,
        out_shape=out_shape,
        in_specs=[pl.BlockSpec(memory_space=spaces[s]) for s in in_spaces],
        out_specs=jax.tree.map(lambda _: pl.BlockSpec(memory_space=pltpu.VMEM), out_shape),
        scratch_shapes=list(scratch),
        compiler_params=pltpu.CompilerParams(vmem_limit_bytes=int(vmem_mib * 2**20)),
        cost_estimate=pl.CostEstimate(flops=flops, bytes_accessed=2**20, transcendentals=0),
    )


def panel_of(ref, slot, cap, kind, column):
    pairs = cap // PAIR
    slots = ref.shape[0] // (2 * pairs)
    first = ((column % 2) * slots + slot) * pairs
    return ref[first : first + pairs, kind + column // 2].reshape(cap, LANES)


def rows_of(ref, slot, cap, kind, columns):
    return jnp.concatenate([panel_of(ref, slot, cap, kind, c) for c in range(columns)], axis=1)


def put_pieces(out_ref, first, rows):
    half = out_ref.shape[0] // 2
    pairs = rows.shape[0] // PAIR
    for h in range(2):
        piece = rows[:, h * LANES : (h + 1) * LANES].reshape(pairs, PAIR, LANES)
        out_ref[h * half + first : h * half + first + pairs] = piece


def move(outer, inner, leads, shifts, src_ref, put, double_ref):
    def widen(o, carry):
        rows = src_ref[pl.ds(o * inner, inner)]
        double_ref[pl.ds(2 * o * inner, inner)] = rows
        double_ref[pl.ds((2 * o + 1) * inner, inner)] = rows
        return carry

    lax.fori_loop(0, outer, widen, 0)

    def rows(o, carry):
        for k, (lead, shift) in enumerate(zip(leads, shifts)):
            start = 2 * o * inner + ((inner - shift) & (inner - 1))
            put(k, ((o + lead) & (outer - 1)) * inner, double_ref[pl.ds(start, inner)])
        return carry

    lax.fori_loop(0, outer, rows, 0)


def deliver_kernel(outer, inner, owner_ref, here_ref, src_ref, out_ref, double_ref):
    owner = owner_ref[here_ref[0]]

    def put(k, first, rows):
        out_ref[pl.ds(first, inner)] = rows

    move(
        outer, inner, [lax.div(owner, inner)], [lax.rem(owner, inner)], src_ref, put, double_ref
    )


def exchange_kernel(outer, inner, slots, owner_ref, here_ref, src_ref, out_ref, double_ref):
    slot = here_ref[0]
    group = lax.div(owner_ref[slot], inner)
    member = lax.rem(owner_ref[slot], inner)
    leads = [outer - group]
    shifts = [inner - member]
    for k in range(1, slots):
        other = owner_ref[lax.rem(slot + k, slots)]
        leads.append(lax.div(other, inner) - group + outer)
        shifts.append((lax.rem(other, inner) - member + inner) & (inner - 1))

    def put(k, first, rows):
        out_ref[pl.ds(first, inner), k] = rows

    move(outer, inner, leads, shifts, src_ref, put, double_ref)


def keep_live(rows, limit):
    row = lax.broadcasted_iota(jnp.int32, rows.shape, 0)
    return jnp.where(row < limit, rows, jnp.zeros_like(rows))


def spread_kernel(got_ref, out_ref):
    sums = jnp.sum(got_ref[...], axis=0, keepdims=True)
    out_ref[...] = jnp.broadcast_to(sums, out_ref.shape)


def huber_scale(sums_ref, entries):
    spread = jnp.sum(sums_ref[:, 0, :], axis=0, keepdims=True)
    return 1.345 * spread[:, 0:1] / entries + 1e-06


def start_kernel(
    cap, ranks_ref, v_hbm_ref, warm_hbm_ref, pieces_ref, v_ref, warm_ref, vt_ref, sems
):
    load_v = pltpu.make_async_copy(v_hbm_ref, v_ref, sems.at[0])
    load_warm = pltpu.make_async_copy(warm_hbm_ref, warm_ref, sems.at[1])
    load_v.start()
    load_warm.start()
    load_v.wait()
    vt_ref[...] = v_ref[...].T
    slots = v_ref.shape[1] // cap
    half = pieces_ref.shape[0] // 2
    pairs = cap // PAIR

    def put(kind, right):
        rows = jnp.dot(vt_ref[...], right, preferred_element_type=F32)
        for t in range(slots):
            for h in range(2):
                part = rows[t * cap : (t + 1) * cap, h * LANES : (h + 1) * LANES]
                part = keep_live(part, ranks_ref[t])
                if kind > 0:
                    column = ((kind - 1) * 2 + h) * LANES
                    lane = lax.broadcasted_iota(jnp.int32, part.shape, 1) + column % cap
                    part = jnp.where(lane < ranks_ref[column // cap], part, jnp.zeros_like(part))
                first = h * half + t * pairs
                pieces_ref[first : first + pairs, kind] = part.astype(BF16).reshape(pairs, PAIR, LANES)

    for kind in range(1, pieces_ref.shape[1]):
        put(kind, v_ref[:, (kind - 1) * 2 * LANES : kind * 2 * LANES])
    load_warm.wait()
    put(0, warm_ref[...])


def first_kernel(
    cap, pieces_ref, u_ref, observed_ref, residual_ref, sums_ref, gram_ref, ut_ref, arrived_ref
):
    ut_ref[...] = u_ref[...].T
    for t in range(u_ref.shape[1] // cap):
        arrived_ref[t * cap : (t + 1) * cap] = rows_of(pieces_ref, t, cap, 0, 2)
        gram_ref[t * cap : (t + 1) * cap] = rows_of(pieces_ref, t, cap, 1, gram_ref.shape[1] // LANES)
    total = jnp.zeros((1, 1), F32)
    step = 256
    for i in range(0, u_ref.shape[0], step):
        rows = jnp.dot(u_ref[i : i + step], arrived_ref[...], preferred_element_type=F32)
        rows = rows - observed_ref[i : i + step].astype(F32)
        residual_ref[i : i + step] = rows
        total = total + jnp.sum(jnp.abs(rows), keepdims=True)
    sums_ref[...] = jnp.broadcast_to(total[None], sums_ref.shape)


def weigh_kernel(entries, sums_ref, residual_ref, ut_ref, pieces_ref, own_ref, weighted_ref):
    scale = huber_scale(sums_ref, entries)
    residual = residual_ref[...]
    weighted_ref[...] = (scale / jnp.maximum(jnp.abs(residual), scale) * residual).astype(BF16)
    step = 256
    for i in range(0, ut_ref.shape[0], step):
        rows = jnp.dot(ut_ref[i : i + step], weighted_ref[...], preferred_element_type=F32)
        rows = rows.astype(BF16)
        own_ref[i : i + step] = rows
        put_pieces(pieces_ref, i // PAIR, rows)


def iterate_kernel(
    cap,
    entries,
    ranks_ref,
    spread_ref,
    pieces_ref,
    own_ref,
    gram_ref,
    v_ref,
    u_ref,
    residual_ref,
    gradient_ref,
    image_ref,
    sums_ref,
    back_ref,
    around_ref,
    panels_ref,
):
    slots = v_ref.shape[1] // cap
    step = 256
    for t in range(slots):
        back_ref[t * cap : (t + 1) * cap] = keep_live(rows_of(pieces_ref, t, cap, 0, 2), ranks_ref[t])
    grad = jnp.zeros((1, 1), F32)
    for i in range(0, v_ref.shape[0], step):
        rows = jnp.dot(v_ref[i : i + step], back_ref[...], preferred_element_type=F32)
        gradient_ref[i : i + step] = rows
        grad = grad + jnp.sum(rows * rows, keepdims=True)
    for mine in range(slots):
        for t in range(slots):
            kind = (mine - t) % slots
            if kind == 0:
                around_ref[t * cap : (t + 1) * cap] = own_ref[t * cap : (t + 1) * cap]
            else:
                around_ref[t * cap : (t + 1) * cap] = rows_of(pieces_ref, t, cap, kind, 2)
        panels_ref[mine * cap : (mine + 1) * cap] = jnp.dot(
            gram_ref[mine * cap : (mine + 1) * cap], around_ref[...], preferred_element_type=F32
        ).astype(BF16)
    scale = huber_scale(spread_ref, entries)
    curve = jnp.zeros((1, 1), F32)
    for i in range(0, u_ref.shape[0], step):
        rows = jnp.dot(u_ref[i : i + step], panels_ref[...], preferred_element_type=F32)
        image_ref[i : i + step] = rows
        weights = scale / jnp.maximum(jnp.abs(residual_ref[i : i + step]), scale)
        curve = curve + jnp.sum(weights * rows * rows, keepdims=True)
    lane = lax.broadcasted_iota(jnp.int32, sums_ref.shape, 2)
    sums_ref[...] = jnp.where(lane < LANES // 2, grad[None], curve[None])


def step_of(sums_ref):
    sums = jnp.sum(sums_ref[:, 0, :], axis=0, keepdims=True)
    return sums[:, 0:1] / (sums[:, LANES // 2 : LANES // 2 + 1] + 1e-06)


def update_kernel(sums_ref, residual_ref, image_ref, out_ref, step_ref, spread_ref):
    step = step_of(sums_ref)
    residual = residual_ref[...] - step * image_ref[...]
    out_ref[...] = residual
    step_ref[...] = jnp.broadcast_to(step, step_ref.shape)
    total = jnp.sum(jnp.abs(residual), keepdims=True)
    spread_ref[...] = jnp.broadcast_to(total[None], spread_ref.shape)


def last_kernel(sums_ref, residual_ref, image_ref, start_ref, gradient_ref, *rest):
    earlier, (out_ref, residual_out_ref) = rest[:-2], rest[-2:]
    step = step_of(sums_ref)
    model = start_ref[...].astype(F32)
    for k in range(0, len(earlier), 2):
        model = model - earlier[k][0:1, 0:1] * earlier[k + 1][...]
    out_ref[...] = model - step * gradient_ref[...]
    residual_out_ref[...] = (residual_ref[...] - step * image_ref[...]).astype(BF16)


def on_device(v_stack, u_stack, warm_start, observed, owners, tile_ranks):
    groups = lax.axis_size(GRP)
    members = lax.axis_size(MEM)
    devices = groups * members
    slots = owners.shape[1]
    block, width = v_stack.shape
    cap = width // slots
    rhs = warm_start.shape[1]
    entries = float(block * rhs * groups * members)
    ranks = tile_ranks[0]
    struct = jax.ShapeDtypeStruct
    field = struct((block, rhs), F32)
    rounded = struct((block, rhs), BF16)
    panels_shape = struct((width, rhs), BF16)
    piece = (PAIR, LANES)
    flops = 2 * block * width * rhs

    half = devices // 2
    slot = lax.axis_index(ALL) % half // (half // slots)
    here = slot[None]
    owner = owners[0]

    def scatter(x, axes):
        return lax.all_to_all(x, axes, split_axis=0, concat_axis=0, tiled=True)

    def route(kernel, pieces, out):
        got = scatter(pieces, ALL)
        moved = call(
            functools.partial(kernel, groups, members),
            struct((devices,) + out, BF16),
            "ssv",
            [pltpu.VMEM((2 * devices,) + pieces.shape[1:], BF16)],
            flops=10**8,
        )(owner, here, got)
        return scatter(moved, ALL)

    def total(partial):
        got = scatter(partial, GRP)
        spread = call(spread_kernel, struct((members, 1, LANES), F32), "v")(got)
        return scatter(spread, MEM)

    kinds = (rhs + width) // (2 * LANES)
    pieces = call(
        functools.partial(start_kernel, cap),
        struct((devices, kinds) + piece, BF16),
        "shh",
        [
            pltpu.VMEM((block, width), BF16),
            pltpu.VMEM((block, rhs), BF16),
            pltpu.VMEM((width, block), BF16),
            pltpu.SemaphoreType.DMA((2,)),
        ],
        flops=3 * flops,
        vmem_mib=60.5,
    )(ranks, v_stack, warm_start)
    one = struct((groups, 1, LANES), F32)
    residual, partial, gram, ut = call(
        functools.partial(first_kernel, cap),
        (field, one, struct((width, width), BF16), struct((width, block), BF16)),
        "vvv",
        [pltpu.VMEM((width, rhs), BF16)],
        flops=flops,
    )(route(deliver_kernel, pieces, (kinds,) + piece), u_stack, observed)
    exchange = lambda outer, inner, *refs: exchange_kernel(outer, inner, slots, *refs)
    earlier = []
    for index in range(ITERS):
        spread = total(partial)
        pieces, own = call(
            functools.partial(weigh_kernel, entries),
            (struct((devices,) + piece, BF16), panels_shape),
            "vvv",
            [pltpu.VMEM((block, rhs), BF16)],
            flops=flops,
        )(spread, residual, ut)
        gradient, image, partial = call(
            functools.partial(iterate_kernel, cap, entries),
            (field, field, one),
            "svvvvvvv",
            [pltpu.VMEM((width, rhs), BF16)] * 3,
            flops=3 * flops,
        )(
            ranks,
            spread,
            route(exchange, pieces, (slots,) + piece),
            own,
            gram,
            v_stack,
            u_stack,
            residual,
        )
        sums = total(partial)
        if index < ITERS - 1:
            residual, step, partial = call(
                update_kernel, (field, struct((8, LANES), F32), one), "vvv"
            )(sums, residual, image)
            earlier += [step, gradient]
        else:
            model, residual = call(last_kernel, (field, rounded), "v" * (5 + len(earlier)))(
                sums, residual, image, warm_start, gradient, *earlier
            )
    return model, residual


def solution(mesh):
    finer = Mesh(mesh.devices.reshape(8, 2, 4, 8), ALL)
    rows = P(ALL, None)
    return jax.shard_map(
        on_device,
        mesh=finer,
        in_specs=(rows, rows, rows, rows, P(), rows),
        out_specs=(rows, rows),
        check_vma=False,
    )
```

```python
import functools

import jax
import jax.numpy as jnp
from jax import lax
from jax.experimental import pallas as pl
from jax.experimental.pallas import tpu as pltpu
from jax.sharding import Mesh
from jax.sharding import PartitionSpec as P

ITERS = 2
ALL = ("y", "c", "x", "z")
GRP = ("y", "c")
MEM = ("x", "z")
LANES = 128
PAIR = 2
F32 = jnp.float32
BF16 = jnp.bfloat16


def call(kernel, out_shape, in_spaces, scratch=(), flops=0, vmem_mib=12):
    spaces = {"v": pltpu.VMEM, "s": pltpu.SMEM, "h": pltpu.HBM}
    return pl.pallas_call(
        kernel,
        out_shape=out_shape,
        in_specs=[pl.BlockSpec(memory_space=spaces[s]) for s in in_spaces],
        out_specs=jax.tree.map(lambda _: pl.BlockSpec(memory_space=pltpu.VMEM), out_shape),
        scratch_shapes=list(scratch),
        compiler_params=pltpu.CompilerParams(vmem_limit_bytes=int(vmem_mib * 2**20)),
        cost_estimate=pl.CostEstimate(flops=flops, bytes_accessed=2**20, transcendentals=0),
    )


def panel_of(ref, slot, cap, kind, column):
    pairs = cap // PAIR
    slots = ref.shape[0] // (2 * pairs)
    first = ((column % 2) * slots + slot) * pairs
    return ref[first : first + pairs, kind + column // 2].reshape(cap, LANES)


def rows_of(ref, slot, cap, kind, columns):
    return jnp.concatenate([panel_of(ref, slot, cap, kind, c) for c in range(columns)], axis=1)


def put_pieces(out_ref, first, rows):
    half = out_ref.shape[0] // 2
    pairs = rows.shape[0] // PAIR
    for h in range(2):
        piece = rows[:, h * LANES : (h + 1) * LANES].reshape(pairs, PAIR, LANES)
        out_ref[h * half + first : h * half + first + pairs] = piece


def widen(outer, inner, src_ref, double_ref):
    def rows(o, carry):
        block = src_ref[pl.ds(o * inner, inner)]
        double_ref[pl.ds(2 * o * inner, inner)] = block
        double_ref[pl.ds((2 * o + 1) * inner, inner)] = block
        return carry

    lax.fori_loop(0, outer, rows, 0)


def arriving(outer, inner, o, lead, shift, double_ref):
    source = (o + outer - lead) & (outer - 1)
    return double_ref[pl.ds(2 * source * inner + ((inner - shift) & (inner - 1)), inner)]


def deliver_kernel(outer, inner, owner_ref, here_ref, src_ref, out_ref, double_ref):
    owner = owner_ref[here_ref[0]]
    lead, shift = lax.div(owner, inner), lax.rem(owner, inner)
    widen(outer, inner, src_ref, double_ref)

    def rows(o, carry):
        out_ref[pl.ds(o * inner, inner)] = arriving(outer, inner, o, lead, shift, double_ref)
        return carry

    lax.fori_loop(0, outer, rows, 0)


def exchange_kernel(outer, inner, slots, owner_ref, here_ref, src_ref, out_ref, double_ref):
    slot = here_ref[0]
    group = lax.div(owner_ref[slot], inner)
    member = lax.rem(owner_ref[slot], inner)
    leads = [(outer - group) & (outer - 1)]
    shifts = [(inner - member) & (inner - 1)]
    for k in range(1, slots):
        other = owner_ref[lax.rem(slot + k, slots)]
        leads.append((lax.div(other, inner) - group + outer) & (outer - 1))
        shifts.append((lax.rem(other, inner) - member + inner) & (inner - 1))
    widen(outer, inner, src_ref, double_ref)

    def rows(o, carry):
        pieces = [
            arriving(outer, inner, o, lead, shift, double_ref) for lead, shift in zip(leads, shifts)
        ]
        out_ref[pl.ds(o * inner, inner)] = jnp.concatenate(pieces, axis=1)
        return carry

    lax.fori_loop(0, outer, rows, 0)


def keep_live(rows, limit):
    row = lax.broadcasted_iota(jnp.int32, rows.shape, 0)
    return jnp.where(row < limit, rows, jnp.zeros_like(rows))


def spread_kernel(got_ref, out_ref):
    sums = jnp.sum(got_ref[...], axis=0, keepdims=True)
    out_ref[...] = jnp.broadcast_to(sums, out_ref.shape)


def huber_scale(sums_ref, entries):
    spread = jnp.sum(sums_ref[:, 0, :], axis=0, keepdims=True)
    return 1.345 * spread[:, 0:1] / entries + 1e-06


def start_kernel(
    cap, ranks_ref, v_hbm_ref, warm_hbm_ref, pieces_ref, v_ref, warm_ref, vt_ref, sems
):
    load_v = pltpu.make_async_copy(v_hbm_ref, v_ref, sems.at[0])
    load_warm = pltpu.make_async_copy(warm_hbm_ref, warm_ref, sems.at[1])
    load_v.start()
    load_warm.start()
    load_v.wait()
    vt_ref[...] = v_ref[...].T
    slots = v_ref.shape[1] // cap
    half = pieces_ref.shape[0] // 2
    pairs = cap // PAIR

    def put(kind, right):
        rows = jnp.dot(vt_ref[...], right, preferred_element_type=F32)
        for t in range(slots):
            for h in range(2):
                part = rows[t * cap : (t + 1) * cap, h * LANES : (h + 1) * LANES]
                part = keep_live(part, ranks_ref[t])
                if kind > 0:
                    column = ((kind - 1) * 2 + h) * LANES
                    lane = lax.broadcasted_iota(jnp.int32, part.shape, 1) + column % cap
                    part = jnp.where(lane < ranks_ref[column // cap], part, jnp.zeros_like(part))
                first = h * half + t * pairs
                pieces_ref[first : first + pairs, kind] = part.astype(BF16).reshape(pairs, PAIR, LANES)

    for kind in range(1, pieces_ref.shape[1]):
        put(kind, v_ref[:, (kind - 1) * 2 * LANES : kind * 2 * LANES])
    load_warm.wait()
    put(0, warm_ref[...])


def first_kernel(
    cap, pieces_ref, u_ref, observed_ref, residual_ref, sums_ref, gram_ref, ut_ref, arrived_ref
):
    ut_ref[...] = u_ref[...].T
    for t in range(u_ref.shape[1] // cap):
        arrived_ref[t * cap : (t + 1) * cap] = rows_of(pieces_ref, t, cap, 0, 2)
        gram_ref[t * cap : (t + 1) * cap] = rows_of(pieces_ref, t, cap, 1, gram_ref.shape[1] // LANES)
    total = jnp.zeros((1, 1), F32)
    step = 256
    for i in range(0, u_ref.shape[0], step):
        rows = jnp.dot(u_ref[i : i + step], arrived_ref[...], preferred_element_type=F32)
        rows = rows - observed_ref[i : i + step].astype(F32)
        residual_ref[i : i + step] = rows
        total = total + jnp.sum(jnp.abs(rows), keepdims=True)
    sums_ref[...] = jnp.broadcast_to(total[None], sums_ref.shape)


def weigh_kernel(entries, sums_ref, residual_ref, ut_ref, pieces_ref, own_ref, weighted_ref):
    scale = huber_scale(sums_ref, entries)
    residual = residual_ref[...]
    weighted_ref[...] = (scale / jnp.maximum(jnp.abs(residual), scale) * residual).astype(BF16)
    step = 256
    for i in range(0, ut_ref.shape[0], step):
        rows = jnp.dot(ut_ref[i : i + step], weighted_ref[...], preferred_element_type=F32)
        rows = rows.astype(BF16)
        own_ref[i : i + step] = rows
        put_pieces(pieces_ref, i // PAIR, rows)


def iterate_kernel(
    cap,
    entries,
    ranks_ref,
    spread_ref,
    pieces_ref,
    own_ref,
    gram_ref,
    v_ref,
    u_ref,
    residual_ref,
    gradient_ref,
    image_ref,
    sums_ref,
    back_ref,
    around_ref,
    panels_ref,
):
    slots = v_ref.shape[1] // cap
    step = 256
    for t in range(slots):
        back_ref[t * cap : (t + 1) * cap] = keep_live(rows_of(pieces_ref, t, cap, 0, 2), ranks_ref[t])
    grad = jnp.zeros((1, 1), F32)
    for i in range(0, v_ref.shape[0], step):
        rows = jnp.dot(v_ref[i : i + step], back_ref[...], preferred_element_type=F32)
        gradient_ref[i : i + step] = rows
        grad = grad + jnp.sum(rows * rows, keepdims=True)
    for mine in range(slots):
        for t in range(slots):
            kind = (mine - t) % slots
            if kind == 0:
                around_ref[t * cap : (t + 1) * cap] = own_ref[t * cap : (t + 1) * cap]
            else:
                around_ref[t * cap : (t + 1) * cap] = rows_of(pieces_ref, t, cap, kind, 2)
        panels_ref[mine * cap : (mine + 1) * cap] = jnp.dot(
            gram_ref[mine * cap : (mine + 1) * cap], around_ref[...], preferred_element_type=F32
        ).astype(BF16)
    scale = huber_scale(spread_ref, entries)
    curve = jnp.zeros((1, 1), F32)
    for i in range(0, u_ref.shape[0], step):
        rows = jnp.dot(u_ref[i : i + step], panels_ref[...], preferred_element_type=F32)
        image_ref[i : i + step] = rows
        weights = scale / jnp.maximum(jnp.abs(residual_ref[i : i + step]), scale)
        curve = curve + jnp.sum(weights * rows * rows, keepdims=True)
    lane = lax.broadcasted_iota(jnp.int32, sums_ref.shape, 2)
    sums_ref[...] = jnp.where(lane < LANES // 2, grad[None], curve[None])


def step_of(sums_ref):
    sums = jnp.sum(sums_ref[:, 0, :], axis=0, keepdims=True)
    return sums[:, 0:1] / (sums[:, LANES // 2 : LANES // 2 + 1] + 1e-06)


def update_kernel(sums_ref, residual_ref, image_ref, out_ref, step_ref, spread_ref):
    step = step_of(sums_ref)
    residual = residual_ref[...] - step * image_ref[...]
    out_ref[...] = residual
    step_ref[...] = jnp.broadcast_to(step, step_ref.shape)
    total = jnp.sum(jnp.abs(residual), keepdims=True)
    spread_ref[...] = jnp.broadcast_to(total[None], spread_ref.shape)


def last_kernel(sums_ref, residual_ref, image_ref, start_ref, gradient_ref, *rest):
    earlier, (out_ref, residual_out_ref) = rest[:-2], rest[-2:]
    step = step_of(sums_ref)
    model = start_ref[...].astype(F32)
    for k in range(0, len(earlier), 2):
        model = model - earlier[k][0:1, 0:1] * earlier[k + 1][...]
    out_ref[...] = model - step * gradient_ref[...]
    residual_out_ref[...] = (residual_ref[...] - step * image_ref[...]).astype(BF16)


def on_device(v_stack, u_stack, warm_start, observed, owners, tile_ranks):
    groups = lax.axis_size(GRP)
    members = lax.axis_size(MEM)
    devices = groups * members
    slots = owners.shape[1]
    block, width = v_stack.shape
    cap = width // slots
    rhs = warm_start.shape[1]
    entries = float(block * rhs * groups * members)
    ranks = tile_ranks[0]
    struct = jax.ShapeDtypeStruct
    field = struct((block, rhs), F32)
    rounded = struct((block, rhs), BF16)
    panels_shape = struct((width, rhs), BF16)
    piece = (PAIR, LANES)
    flops = 2 * block * width * rhs

    half = devices // 2
    slot = lax.axis_index(ALL) % half // (half // slots)
    here = slot[None]
    owner = owners[0]

    def scatter(x, axes):
        return lax.all_to_all(x, axes, split_axis=0, concat_axis=0, tiled=True)

    def route(kernel, pieces, out):
        got = scatter(pieces, ALL)
        moved = call(
            functools.partial(kernel, groups, members),
            struct((devices,) + out, BF16),
            "ssv",
            [pltpu.VMEM((2 * devices,) + pieces.shape[1:], BF16)],
            flops=10**8,
        )(owner, here, got)
        return scatter(moved, ALL)

    def total(partial):
        got = scatter(partial, GRP)
        spread = call(spread_kernel, struct((members, 1, LANES), F32), "v")(got)
        return scatter(spread, MEM)

    kinds = (rhs + width) // (2 * LANES)
    pieces = call(
        functools.partial(start_kernel, cap),
        struct((devices, kinds) + piece, BF16),
        "shh",
        [
            pltpu.VMEM((block, width), BF16),
            pltpu.VMEM((block, rhs), BF16),
            pltpu.VMEM((width, block), BF16),
            pltpu.SemaphoreType.DMA((2,)),
        ],
        flops=3 * flops,
        vmem_mib=60.5,
    )(ranks, v_stack, warm_start)
    one = struct((groups, 1, LANES), F32)
    residual, partial, gram, ut = call(
        functools.partial(first_kernel, cap),
        (field, one, struct((width, width), BF16), struct((width, block), BF16)),
        "vvv",
        [pltpu.VMEM((width, rhs), BF16)],
        flops=flops,
    )(route(deliver_kernel, pieces, (kinds,) + piece), u_stack, observed)
    exchange = lambda outer, inner, *refs: exchange_kernel(outer, inner, slots, *refs)
    earlier = []
    for index in range(ITERS):
        spread = total(partial)
        pieces, own = call(
            functools.partial(weigh_kernel, entries),
            (struct((devices,) + piece, BF16), panels_shape),
            "vvv",
            [pltpu.VMEM((block, rhs), BF16)],
            flops=flops,
        )(spread, residual, ut)
        gradient, image, partial = call(
            functools.partial(iterate_kernel, cap, entries),
            (field, field, one),
            "svvvvvvv",
            [pltpu.VMEM((width, rhs), BF16)] * 3,
            flops=3 * flops,
        )(
            ranks,
            spread,
            route(exchange, pieces, (slots * PAIR, LANES)).reshape((devices, slots) + piece),
            own,
            gram,
            v_stack,
            u_stack,
            residual,
        )
        sums = total(partial)
        if index < ITERS - 1:
            residual, step, partial = call(
                update_kernel, (field, struct((8, LANES), F32), one), "vvv"
            )(sums, residual, image)
            earlier += [step, gradient]
        else:
            model, residual = call(last_kernel, (field, rounded), "v" * (5 + len(earlier)))(
                sums, residual, image, warm_start, gradient, *earlier
            )
    return model, residual


def solution(mesh):
    finer = Mesh(mesh.devices.reshape(8, 2, 4, 8), ALL)
    rows = P(ALL, None)
    return jax.shard_map(
        on_device,
        mesh=finer,
        in_specs=(rows, rows, rows, rows, P(), rows),
        out_specs=(rows, rows),
        check_vma=False,
    )
```

```python
import functools

import jax
import jax.numpy as jnp
from jax import lax
from jax.experimental import pallas as pl
from jax.experimental.pallas import tpu as pltpu
from jax.sharding import Mesh
from jax.sharding import PartitionSpec as P

ITERS = 2
ALL = ("y", "c", "x", "z")
GRP = ("y", "c")
MEM = ("x", "z")
LANES = 128
PAIR = 2
F32 = jnp.float32
BF16 = jnp.bfloat16


def call(kernel, out_shape, in_spaces, scratch=(), flops=0, vmem_mib=12):
    spaces = {"v": pltpu.VMEM, "s": pltpu.SMEM, "h": pltpu.HBM}
    return pl.pallas_call(
        kernel,
        out_shape=out_shape,
        in_specs=[pl.BlockSpec(memory_space=spaces[s]) for s in in_spaces],
        out_specs=jax.tree.map(lambda _: pl.BlockSpec(memory_space=pltpu.VMEM), out_shape),
        scratch_shapes=list(scratch),
        compiler_params=pltpu.CompilerParams(vmem_limit_bytes=int(vmem_mib * 2**20)),
        cost_estimate=pl.CostEstimate(flops=flops, bytes_accessed=2**20, transcendentals=0),
    )


def panel_of(ref, slot, cap, kind, column):
    pairs = cap // PAIR
    slots = ref.shape[0] // (2 * pairs)
    first = ((column % 2) * slots + slot) * pairs
    return ref[first : first + pairs, kind + column // 2].reshape(cap, LANES)


def rows_of(ref, slot, cap, kind, columns):
    return jnp.concatenate([panel_of(ref, slot, cap, kind, c) for c in range(columns)], axis=1)


def put_pieces(out_ref, first, rows):
    half = out_ref.shape[0] // 2
    pairs = rows.shape[0] // PAIR
    for h in range(2):
        piece = rows[:, h * LANES : (h + 1) * LANES].reshape(pairs, PAIR, LANES)
        out_ref[h * half + first : h * half + first + pairs] = piece


def widen(outer, inner, src_ref, double_ref):
    def rows(o, carry):
        block = src_ref[pl.ds(o * inner, inner)]
        double_ref[pl.ds(2 * o * inner, inner)] = block
        double_ref[pl.ds((2 * o + 1) * inner, inner)] = block
        return carry

    lax.fori_loop(0, outer, rows, 0)


def arriving(outer, inner, o, lead, shift, double_ref):
    source = (o + outer - lead) & (outer - 1)
    return double_ref[pl.ds(2 * source * inner + ((inner - shift) & (inner - 1)), inner)]


def deliver_kernel(outer, inner, owner_ref, here_ref, src_ref, ranks_ref, out_ref, double_ref):
    owner = owner_ref[here_ref[0]]
    lead, shift = lax.div(owner, inner), lax.rem(owner, inner)
    widen(outer, inner, src_ref, double_ref)

    def rows(o, carry):
        out_ref[pl.ds(o * inner, inner)] = arriving(outer, inner, o, lead, shift, double_ref)
        return carry

    lax.fori_loop(0, outer, rows, 0)


def exchange_kernel(outer, inner, slots, owner_ref, here_ref, src_ref, out_ref, double_ref):
    slot = here_ref[0]
    group = lax.div(owner_ref[slot], inner)
    member = lax.rem(owner_ref[slot], inner)
    leads = [(outer - group) & (outer - 1)]
    shifts = [(inner - member) & (inner - 1)]
    for k in range(1, slots):
        other = owner_ref[lax.rem(slot + k, slots)]
        leads.append((lax.div(other, inner) - group + outer) & (outer - 1))
        shifts.append((lax.rem(other, inner) - member + inner) & (inner - 1))
    widen(outer, inner, src_ref, double_ref)

    def rows(o, carry):
        pieces = [
            arriving(outer, inner, o, lead, shift, double_ref) for lead, shift in zip(leads, shifts)
        ]
        out_ref[pl.ds(o * inner, inner)] = jnp.concatenate(pieces, axis=1)
        return carry

    lax.fori_loop(0, outer, rows, 0)


def keep_live(rows, limit):
    row = lax.broadcasted_iota(jnp.int32, rows.shape, 0)
    return jnp.where(row < limit, rows, jnp.zeros_like(rows))


def spread_kernel(got_ref, out_ref):
    sums = jnp.sum(got_ref[...], axis=0, keepdims=True)
    out_ref[...] = jnp.broadcast_to(sums, out_ref.shape)


def huber_scale(sums_ref, entries):
    spread = jnp.sum(sums_ref[:, 0, :], axis=0, keepdims=True)
    return 1.345 * spread[:, 0:1] / entries + 1e-06


def start_kernel(
    cap, ranks_ref, v_hbm_ref, warm_hbm_ref, pieces_ref, v_ref, warm_ref, vt_ref, sems
):
    load_v = pltpu.make_async_copy(v_hbm_ref, v_ref, sems.at[0])
    load_warm = pltpu.make_async_copy(warm_hbm_ref, warm_ref, sems.at[1])
    load_v.start()
    load_warm.start()
    load_v.wait()
    vt_ref[...] = v_ref[...].T
    slots = v_ref.shape[1] // cap
    half = pieces_ref.shape[0] // 2
    pairs = cap // PAIR

    def put(kind, right):
        rows = jnp.dot(vt_ref[...], right, preferred_element_type=F32)
        for t in range(slots):
            for h in range(2):
                part = rows[t * cap : (t + 1) * cap, h * LANES : (h + 1) * LANES]
                part = keep_live(part, ranks_ref[t])
                if kind > 0:
                    column = ((kind - 1) * 2 + h) * LANES
                    lane = lax.broadcasted_iota(jnp.int32, part.shape, 1) + column % cap
                    part = jnp.where(lane < ranks_ref[column // cap], part, jnp.zeros_like(part))
                first = h * half + t * pairs
                pieces_ref[first : first + pairs, kind] = part.astype(BF16).reshape(pairs, PAIR, LANES)

    for kind in range(1, pieces_ref.shape[1]):
        put(kind, v_ref[:, (kind - 1) * 2 * LANES : kind * 2 * LANES])
    load_warm.wait()
    put(0, warm_ref[...])


def first_kernel(
    cap, pieces_ref, u_ref, observed_ref, residual_ref, sums_ref, gram_ref, ut_ref, arrived_ref
):
    ut_ref[...] = u_ref[...].T
    for t in range(u_ref.shape[1] // cap):
        arrived_ref[t * cap : (t + 1) * cap] = rows_of(pieces_ref, t, cap, 0, 2)
        gram_ref[t * cap : (t + 1) * cap] = rows_of(pieces_ref, t, cap, 1, gram_ref.shape[1] // LANES)
    total = jnp.zeros((1, 1), F32)
    step = 256
    for i in range(0, u_ref.shape[0], step):
        rows = jnp.dot(u_ref[i : i + step], arrived_ref[...], preferred_element_type=F32)
        rows = rows - observed_ref[i : i + step].astype(F32)
        residual_ref[i : i + step] = rows
        total = total + jnp.sum(jnp.abs(rows), keepdims=True)
    sums_ref[...] = jnp.broadcast_to(total[None], sums_ref.shape)


def weigh_kernel(entries, sums_ref, residual_ref, ut_ref, pieces_ref, own_ref, weighted_ref):
    scale = huber_scale(sums_ref, entries)
    residual = residual_ref[...]
    weighted_ref[...] = (scale / jnp.maximum(jnp.abs(residual), scale) * residual).astype(BF16)
    step = 256
    for i in range(0, ut_ref.shape[0], step):
        rows = jnp.dot(ut_ref[i : i + step], weighted_ref[...], preferred_element_type=F32)
        rows = rows.astype(BF16)
        own_ref[i : i + step] = rows
        put_pieces(pieces_ref, i // PAIR, rows)


def iterate_kernel(
    cap,
    entries,
    ranks_ref,
    spread_ref,
    pieces_ref,
    own_ref,
    gram_ref,
    v_ref,
    u_ref,
    residual_ref,
    gradient_ref,
    image_ref,
    sums_ref,
    back_ref,
    around_ref,
    panels_ref,
):
    slots = v_ref.shape[1] // cap
    step = 256
    for t in range(slots):
        back_ref[t * cap : (t + 1) * cap] = keep_live(rows_of(pieces_ref, t, cap, 0, 2), ranks_ref[t])
    grad = jnp.zeros((1, 1), F32)
    for i in range(0, v_ref.shape[0], step):
        rows = jnp.dot(v_ref[i : i + step], back_ref[...], preferred_element_type=F32)
        gradient_ref[i : i + step] = rows
        grad = grad + jnp.sum(rows * rows, keepdims=True)
    for mine in range(slots):
        for t in range(slots):
            kind = (mine - t) % slots
            if kind == 0:
                around_ref[t * cap : (t + 1) * cap] = own_ref[t * cap : (t + 1) * cap]
            else:
                around_ref[t * cap : (t + 1) * cap] = rows_of(pieces_ref, t, cap, kind, 2)
        panels_ref[mine * cap : (mine + 1) * cap] = jnp.dot(
            gram_ref[mine * cap : (mine + 1) * cap], around_ref[...], preferred_element_type=F32
        ).astype(BF16)
    scale = huber_scale(spread_ref, entries)
    curve = jnp.zeros((1, 1), F32)
    for i in range(0, u_ref.shape[0], step):
        rows = jnp.dot(u_ref[i : i + step], panels_ref[...], preferred_element_type=F32)
        image_ref[i : i + step] = rows
        weights = scale / jnp.maximum(jnp.abs(residual_ref[i : i + step]), scale)
        curve = curve + jnp.sum(weights * rows * rows, keepdims=True)
    lane = lax.broadcasted_iota(jnp.int32, sums_ref.shape, 2)
    sums_ref[...] = jnp.where(lane < LANES // 2, grad[None], curve[None])


def step_of(sums_ref):
    sums = jnp.sum(sums_ref[:, 0, :], axis=0, keepdims=True)
    return sums[:, 0:1] / (sums[:, LANES // 2 : LANES // 2 + 1] + 1e-06)


def update_kernel(sums_ref, residual_ref, image_ref, out_ref, step_ref, spread_ref):
    step = step_of(sums_ref)
    residual = residual_ref[...] - step * image_ref[...]
    out_ref[...] = residual
    step_ref[...] = jnp.broadcast_to(step, step_ref.shape)
    total = jnp.sum(jnp.abs(residual), keepdims=True)
    spread_ref[...] = jnp.broadcast_to(total[None], spread_ref.shape)


def last_kernel(sums_ref, residual_ref, image_ref, start_ref, gradient_ref, *rest):
    earlier, (out_ref, residual_out_ref) = rest[:-2], rest[-2:]
    step = step_of(sums_ref)
    model = start_ref[...].astype(F32)
    for k in range(0, len(earlier), 2):
        model = model - earlier[k][0:1, 0:1] * earlier[k + 1][...]
    out_ref[...] = model - step * gradient_ref[...]
    residual_out_ref[...] = (residual_ref[...] - step * image_ref[...]).astype(BF16)


def on_device(v_stack, u_stack, warm_start, observed, owners, tile_ranks):
    groups = lax.axis_size(GRP)
    members = lax.axis_size(MEM)
    devices = groups * members
    slots = owners.shape[1]
    block, width = v_stack.shape
    cap = width // slots
    rhs = warm_start.shape[1]
    entries = float(block * rhs * groups * members)
    ranks = tile_ranks[0]
    struct = jax.ShapeDtypeStruct
    field = struct((block, rhs), F32)
    rounded = struct((block, rhs), BF16)
    panels_shape = struct((width, rhs), BF16)
    piece = (PAIR, LANES)
    flops = 2 * block * width * rhs

    half = devices // 2
    slot = lax.axis_index(ALL) % half // (half // slots)
    here = slot[None]
    owner = owners[0]

    def scatter(x, axes):
        return lax.all_to_all(x, axes, split_axis=0, concat_axis=0, tiled=True)

    def route(kernel, pieces, out, early=()):
        got = scatter(pieces, ALL)
        moved = call(
            functools.partial(kernel, groups, members),
            struct((devices,) + out, BF16),
            "ssv" + "s" * len(early),
            [pltpu.VMEM((2 * devices,) + pieces.shape[1:], BF16)],
            flops=10**8,
        )(owner, here, got, *early)
        return scatter(moved, ALL)

    def total(partial):
        got = scatter(partial, GRP)
        spread = call(spread_kernel, struct((members, 1, LANES), F32), "v")(got)
        return scatter(spread, MEM)

    kinds = (rhs + width) // (2 * LANES)
    pieces = call(
        functools.partial(start_kernel, cap),
        struct((devices, kinds) + piece, BF16),
        "shh",
        [
            pltpu.VMEM((block, width), BF16),
            pltpu.VMEM((block, rhs), BF16),
            pltpu.VMEM((width, block), BF16),
            pltpu.SemaphoreType.DMA((2,)),
        ],
        flops=3 * flops,
        vmem_mib=60.5,
    )(ranks, v_stack, warm_start)
    one = struct((groups, 1, LANES), F32)
    residual, partial, gram, ut = call(
        functools.partial(first_kernel, cap),
        (field, one, struct((width, width), BF16), struct((width, block), BF16)),
        "vvv",
        [pltpu.VMEM((width, rhs), BF16)],
        flops=flops,
    )(route(deliver_kernel, pieces, (kinds,) + piece, (ranks,)), u_stack, observed)
    exchange = lambda outer, inner, *refs: exchange_kernel(outer, inner, slots, *refs)
    earlier = []
    for index in range(ITERS):
        spread = total(partial)
        pieces, own = call(
            functools.partial(weigh_kernel, entries),
            (struct((devices,) + piece, BF16), panels_shape),
            "vvv",
            [pltpu.VMEM((block, rhs), BF16)],
            flops=flops,
        )(spread, residual, ut)
        gradient, image, partial = call(
            functools.partial(iterate_kernel, cap, entries),
            (field, field, one),
            "svvvvvvv",
            [pltpu.VMEM((width, rhs), BF16)] * 3,
            flops=3 * flops,
        )(
            ranks,
            spread,
            route(exchange, pieces, (slots * PAIR, LANES)).reshape((devices, slots) + piece),
            own,
            gram,
            v_stack,
            u_stack,
            residual,
        )
        sums = total(partial)
        if index < ITERS - 1:
            residual, step, partial = call(
                update_kernel, (field, struct((8, LANES), F32), one), "vvv"
            )(sums, residual, image)
            earlier += [step, gradient]
        else:
            model, residual = call(last_kernel, (field, rounded), "v" * (5 + len(earlier)))(
                sums, residual, image, warm_start, gradient, *earlier
            )
    return model, residual


def solution(mesh):
    finer = Mesh(mesh.devices.reshape(8, 2, 4, 8), ALL)
    rows = P(ALL, None)
    return jax.shard_map(
        on_device,
        mesh=finer,
        in_specs=(rows, rows, rows, rows, P(), rows),
        out_specs=(rows, rows),
        check_vma=False,
    )
```
